32 devices in a mesh: dp: 4 (over y, x), expert: 8 (over z, core).
Axes of the slice: x: 2, y: 2, z: 4, core: 2. Of those that a mesh axis runs over, the one named last changes fastest.
Arguments:
- acts: bfloat16 [8, 512, 2560], P('expert', 'dp'), may hold values from -6 to 6
- out_grads: bfloat16 [8, 512, 768], P('expert', 'dp'), may hold values from -2 to 2
- next_tokens: bfloat16 [8, 512, 2560], P('expert', 'dp'), may hold values from -6 to 6
- master: float32 [8, 2560, 768], P('expert', 'dp'), may hold values from -0.125 to 0.125
- first_moment: float32 [8, 2560, 768], P('expert', 'dp'), may hold values from -6 to 6
- second_moment: float32 [8, 2560, 768], P('expert', 'dp'), may hold values from 0.5 to 20
- counts: int32 [4, 160], P('dp'), may hold values from 32 to 128
- selected: int32 [8], replicated, may hold values from 0 to 159
- old_place: int32 [8], replicated, may hold values from 0 to 7, each once
- new_place: int32 [8], replicated, may hold values from 0 to 7, each once
Outputs:
- new_master: float32 [8, 2560, 768], P('expert', 'dp')
- new_first: float32 [8, 2560, 768], P('expert', 'dp')
- new_second: float32 [8, 2560, 768], P('expert', 'dp')
- forward: bfloat16 [8, 512, 768], P('expert', 'dp')
The draws below stay inside these ranges and needn't reach their ends.
Inputs may be any that keep to these rules, and one draw needn't show every extreme that they name: `old_place`: each holder index appears once. `new_place`: each holder index appears once.
All inputs are finite; a program needn't handle non-finite values.
Results may differ from the reference program's by a relative error of at most 0.012.
Values may be sent and summed in bfloat16 or wider, within the bound.
No kernel may reach another device: no remote copies, remote signals or barrier semaphores. Data moves between devices by JAX's collectives and lax.ppermute only.
A program may use at most 64 MiB of HBM per device.

```python
import math
import jax
import jax.numpy as jnp
from jax import lax

D = 2560
FF = 768
EXPERTS = 160
TOK_DEV = 128
SLOTS = 8
TOKENS = 512
N_DP = 4


def plant(drawn, rng, smallest, high):
    place = [jax.random.randint(jax.random.fold_in(rng, axis), (), 0, length) for axis, length in enumerate(drawn.shape)]
    longest = drawn.shape.index(max(drawn.shape))
    neighbour = place[:longest] + [(place[longest] + 1) % drawn.shape[longest]] + place[longest + 1:]
    return drawn.at[tuple(place)].set(smallest).at[tuple(neighbour)].set(high)


def block_scale(key, extent, pieces, least, top_value):
    def one(axis_at, shards_of):
        heights = jax.random.uniform(jax.random.fold_in(jax.random.fold_in(key, 6), axis_at), (shards_of,), jnp.float32, least / len(pieces), top_value / len(pieces))
        return jnp.repeat(jnp.exp(heights), extent[axis_at] // shards_of).reshape((-1,) + (1,) * (len(extent) - axis_at - 1))

    level = one(*pieces[0])
    for cut in pieces[1:]:
        level = level * one(*cut)
    return level


def centred(own_key, dims, spread, limit, cuts=(), kind=jnp.bfloat16):
    loudness = block_scale(own_key, dims, cuts, -0.22, 0.18) if cuts else 1.0
    values = jax.random.normal(own_key, dims, jnp.float32) * spread * loudness
    return jnp.minimum(jnp.maximum(values, -limit), limit).astype(kind)


def setup_inputs(seed: int = 0) -> dict:
    splits = jax.random.split(jax.random.key(seed), 11)
    return {
        "acts": centred(splits[0], (SLOTS, TOKENS, D), 1.0, 6.0, ((0, 8), (1, 4))),
        "out_grads": centred(splits[1], (SLOTS, TOKENS, FF), (3.0 / TOKENS ** 0.5), 2.0, ((0, 8), (1, 4))),
        "next_tokens": centred(splits[2], (SLOTS, TOKENS, D), 1.0, 6.0, ((0, 8), (1, 4))),
        "master": centred(splits[3], (SLOTS, D, FF), D ** -0.5, 0.125, ((0, 8), (1, 4)), jnp.float32),
        "first_moment": centred(splits[4], (SLOTS, D, FF), 1.0, 6.0, ((0, 8), (1, 4)), jnp.float32),
        "second_moment": jnp.clip(jnp.exp(math.log(20.0) - 3.6888795 * jax.random.uniform(splits[5], (SLOTS, D, FF), jnp.float32) ** block_scale(splits[5], (SLOTS, D, FF), ((0, 8), (1, 4)), -0.2, 0.2)), 0.5, 20.0),
        "counts": plant(jax.random.randint(splits[6], (N_DP, EXPERTS), TOK_DEV // 4, TOK_DEV + 1), jax.random.fold_in(splits[6], 1), TOK_DEV // 4, TOK_DEV).astype(jnp.int32),
        "selected": plant(jax.random.randint(splits[7], (SLOTS,), 0, EXPERTS), jax.random.fold_in(splits[7], 1), 0, EXPERTS - 1).astype(jnp.int32),
        "old_place": jax.random.permutation(splits[8], SLOTS).astype(jnp.int32),
        "new_place": jax.random.permutation(splits[9], SLOTS).astype(jnp.int32),
    }


beta_first = 0.9
beta_second = 0.95
bias_first = 1.0 - 0.9 ** 10
bias_second = 1.0 - 0.95 ** 10
learn_rate = 0.01
decay_rate = 0.1
epsilon = 1e-08

def adamw(weights, moment_one, moment_two, gradient):
    moment_one = beta_first * moment_one + (1.0 - beta_first) * gradient
    moment_two = beta_second * moment_two + (1.0 - beta_second) * gradient * gradient
    update = moment_one / bias_first / (jnp.sqrt(moment_two / bias_second) + epsilon) + decay_rate * weights
    return (weights - learn_rate * update, moment_one, moment_two)

def reference(acts, out_grads, next_tokens, master, first_moment, second_moment, counts, selected, old_place, new_place):
    slots = jnp.arange(SLOTS, dtype=jnp.int32)
    holder = lax.optimization_barrier(jnp.sum(jnp.where(old_place[None, :] == slots[:, None], slots[None, :], 0), axis=1)).astype(jnp.int32)
    expert_of = selected[holder]
    routed = jnp.take(counts, expert_of, axis=1).T

    def gradient_of(packed):
        tokens_in, grads_in, routed_in = packed
        live = jnp.arange(TOK_DEV, dtype=jnp.int32)[None, :] < routed_in[:, None]
        grads_in = grads_in.reshape(N_DP, TOK_DEV, FF)
        masked = jnp.where(live[:, :, None], grads_in, jnp.zeros_like(grads_in))
        blocks = jnp.einsum('stk,stf->skf', tokens_in.reshape(N_DP, TOK_DEV, D).astype(jnp.float32), masked.astype(jnp.float32))
        rounded = lax.optimization_barrier(blocks.astype(jnp.bfloat16))
        return lax.optimization_barrier(jnp.sum(rounded.astype(jnp.float32), axis=0))
    gradients = lax.map(gradient_of, (acts, out_grads, routed))
    weights, moment_one, moment_two = adamw(master, first_moment, second_moment, gradients)
    inverse = lax.optimization_barrier(jnp.sum(jnp.where(new_place[None, :] == slots[:, None], slots[None, :], 0), axis=1)).astype(jnp.int32)
    source = old_place[inverse]
    weights = jnp.take(weights, source, axis=0)
    moment_one = jnp.take(moment_one, source, axis=0)
    moment_two = jnp.take(moment_two, source, axis=0)
    lowered = weights.astype(jnp.bfloat16)

    def forward_of(packed):
        tokens_in, weight_in = packed
        return jnp.dot(tokens_in, weight_in, preferred_element_type=jnp.float32).astype(jnp.bfloat16)
    forward = lax.map(forward_of, (next_tokens, lowered))
    return (weights, moment_one, moment_two, forward)
```

```python
import itertools
import math

import jax
import jax.numpy as jnp
from jax import lax
from jax.sharding import PartitionSpec as P

beta_first = 0.9
beta_second = 0.95
bias_first = 1.0 - 0.9**10
bias_second = 1.0 - 0.95**10
learn_rate = 0.01
decay_rate = 0.1
epsilon = 1e-08

CORES = 2
ROUTE_LIMIT = 24


def adamw(weights, moment_one, moment_two, gradient):
    moment_one = beta_first * moment_one + (1.0 - beta_first) * gradient
    moment_two = beta_second * moment_two + (1.0 - beta_second) * gradient * gradient
    update = (
        moment_one / bias_first / (jnp.sqrt(moment_two / bias_second) + epsilon)
        + decay_rate * weights
    )
    return (weights - learn_rate * update, moment_one, moment_two)


def pick(table, index):
    slots = jnp.arange(table.shape[0], dtype=jnp.int32)
    return jnp.sum(jnp.where(index[..., None] == slots, table, 0), axis=-1)


def some_colouring(destination, source, holders):
    every = jnp.arange(holders, dtype=jnp.int32)
    beside = every ^ 1
    hop = pick(source, pick(destination, beside) ^ 1)
    least = every
    for _ in range(holders // CORES - 1):
        least = jnp.minimum(every, pick(least, hop))
    return (least > pick(least, beside)).astype(jnp.int32)


def rank_of(perm):
    size = perm.shape[0]
    slots = jnp.arange(size, dtype=jnp.int32)
    smaller = jnp.sum(
        jnp.where(
            (perm[None, :] < perm[:, None]) & (slots[None, :] > slots[:, None]), 1, 0
        ),
        axis=1,
    )
    weight = jnp.array([math.factorial(size - 1 - i) for i in range(size)], jnp.int32)
    return jnp.sum(smaller * weight)


def busiest(perm):
    return max(
        max(
            sum(src <= cut < dst for src, dst in enumerate(perm)),
            sum(dst <= cut < src for src, dst in enumerate(perm)),
        )
        for cut in range(len(perm))
    )


def best_pairs(chips):
    orders = list(itertools.permutations(range(chips)))
    best = {}
    codes = []
    for one, two in itertools.product(orders, repeat=CORES):
        traffic = tuple(tuple(sorted(ends)) for ends in zip(one, two))
        codes.append(traffic)
        cost = busiest(one) + busiest(two)
        code = orders.index(one) * len(orders) + orders.index(two)
        best[traffic] = min(best.get(traffic, (cost, code)), (cost, code))
    return orders, [best[traffic][1] for traffic in codes]


def direct_body(
    acts,
    out_grads,
    next_tokens,
    master,
    first_moment,
    second_moment,
    counts,
    selected,
    old_place,
    new_place,
):
    holders = lax.axis_size("expert")
    groups = lax.axis_size("dp")
    me = lax.axis_index("expert")
    chips = holders // CORES
    beside = [(i, i ^ 1) for i in range(holders)]
    tokens_here = acts[0]
    grads_here = out_grads[0]
    rows_each = tokens_here.shape[0]
    shard_rows, width = master.shape[1:]
    half = shard_rows // CORES
    positions = jnp.arange(holders, dtype=jnp.int32)
    expert_id = jnp.sum(jnp.where(old_place == me, selected, 0))
    table = jnp.arange(counts.shape[1], dtype=jnp.int32)
    routed = jnp.sum(jnp.where(table == expert_id, counts[0], 0))
    live = jnp.arange(rows_each, dtype=jnp.int32) < routed
    masked = jnp.where(live[:, None], grads_here, jnp.zeros_like(grads_here))

    packed = jnp.concatenate(
        [
            tokens_here.reshape(rows_each, groups, shard_rows).transpose(1, 0, 2),
            jnp.broadcast_to(masked, (groups, rows_each, width)),
        ],
        axis=2,
    )
    packed = lax.all_to_all(packed, "dp", split_axis=0, concat_axis=0, tiled=True)
    next_columns = lax.all_to_all(
        next_tokens[0].reshape(rows_each, groups, shard_rows).transpose(1, 0, 2),
        "dp",
        split_axis=0,
        concat_axis=0,
        tiled=True,
    )

    destination = jnp.sum(
        jnp.where(old_place[None, :] == positions[:, None], new_place[None, :], 0), axis=1
    )
    source = jnp.sum(
        jnp.where(new_place[None, :] == positions[:, None], old_place[None, :], 0), axis=1
    )
    orders, best = best_pairs(chips)
    chip_slots = jnp.arange(chips, dtype=jnp.int32)
    edge = CORES * chip_slots
    edge = edge + pick(some_colouring(destination, source, holders), edge)
    code = rank_of(pick(destination, edge) // CORES) * len(orders) + rank_of(
        pick(destination, edge ^ 1) // CORES
    )
    code = pick(jnp.array(best, jnp.int32), code[None])[0]
    route_one = code // len(orders)
    route_two = code % len(orders)
    flat_orders = jnp.array(orders, jnp.int32).reshape(-1)
    to_one = pick(flat_orders, route_one * chips + chip_slots)
    rider = CORES * chip_slots + (
        pick(destination, CORES * chip_slots) // CORES != to_one
    ).astype(jnp.int32)
    chip = me // CORES
    core = me % CORES
    sends_one = pick(rider, chip[None])[0] == me
    gets_one = jnp.sum(jnp.where(pick(destination, rider) == me, 1, 0)) > 0

    gradient = jnp.einsum(
        "stk,stf->kf",
        packed[:, :, :shard_rows],
        packed[:, :, shard_rows:],
        preferred_element_type=jnp.float32,
    )
    states = adamw(master[0], first_moment[0], second_moment[0], gradient)
    states = jnp.stack([member.astype(jnp.bfloat16) for member in states])
    keep = lax.dynamic_slice_in_dim(states, core * half, half, axis=1)
    give = lax.dynamic_slice_in_dim(states, (1 - core) * half, half, axis=1)
    take = lax.ppermute(give, "expert", beside)
    one = jnp.where(sends_one, keep, take)
    two = jnp.where(sends_one, take, keep)

    def pairs(order):
        return [
            (z * CORES + c, order[z] * CORES + c)
            for z in range(chips)
            for c in range(CORES)
        ]

    def leg(order):
        return lambda value: lax.ppermute(value, "expert", pairs(order))

    one, two, route_one, route_two = lax.optimization_barrier(
        (one, two, route_one, route_two)
    )
    one = lax.switch(route_one, [leg(order) for order in orders], one)
    one, two = lax.optimization_barrier((one, two))
    two = lax.switch(route_two, [leg(order) for order in orders], two)
    one, two = lax.optimization_barrier((one, two))

    def join(index):
        mine = jnp.where(gets_one, one[index], two[index])
        other = jnp.where(gets_one, two[index], one[index])
        other = lax.ppermute(other, "expert", beside)
        return jnp.where(
            core == 0,
            jnp.concatenate([mine, other], axis=0),
            jnp.concatenate([other, mine], axis=0),
        )

    arrived = [join(index) for index in range(3)]
    partial = jnp.einsum(
        "stk,kf->stf", next_columns, arrived[0], preferred_element_type=jnp.float32
    ).astype(jnp.bfloat16)
    partial = lax.all_to_all(partial, "dp", split_axis=0, concat_axis=0, tiled=True)
    forward = jnp.sum(partial.astype(jnp.float32), axis=0)
    return (
        arrived[0].astype(jnp.float32)[None],
        arrived[1].astype(jnp.float32)[None],
        arrived[2].astype(jnp.float32)[None],
        forward.astype(jnp.bfloat16)[None],
    )


def relocate_states(weights, moment_one, moment_two, order):
    holders = lax.axis_size("expert")
    shard_rows, width = weights.shape
    first = weights.reshape(holders, shard_rows // holders, width)
    second = moment_one.reshape(holders, shard_rows // holders, width)
    third = moment_two.reshape(holders, shard_rows // holders, width)
    relayed = (
        lax.all_to_all(
            first.astype(jnp.bfloat16), "expert", split_axis=0, concat_axis=0, tiled=True
        ).astype(first.dtype),
        lax.all_to_all(
            second.astype(jnp.bfloat16), "expert", split_axis=0, concat_axis=0, tiled=True
        ).astype(second.dtype),
        lax.all_to_all(
            third.astype(jnp.bfloat16), "expert", split_axis=0, concat_axis=0, tiled=True
        ).astype(third.dtype),
    )
    arranged = tuple((jnp.take(member, order, axis=0) for member in relayed))
    arrived = (
        lax.all_to_all(
            arranged[0].astype(jnp.bfloat16), "expert", split_axis=0, concat_axis=0, tiled=True
        ).astype(jnp.float32),
        lax.all_to_all(
            arranged[1].astype(jnp.bfloat16), "expert", split_axis=0, concat_axis=0, tiled=True
        ).astype(jnp.float32),
        lax.all_to_all(
            arranged[2].astype(jnp.bfloat16), "expert", split_axis=0, concat_axis=0, tiled=True
        ).astype(jnp.float32),
    )
    return tuple((member.reshape(shard_rows, width) for member in arrived))


def relay_body(
    acts,
    out_grads,
    next_tokens,
    master,
    first_moment,
    second_moment,
    counts,
    selected,
    old_place,
    new_place,
):
    holders = lax.axis_size("expert")
    my_holder = lax.axis_index("expert")
    tokens_here = acts[0]
    grads_here = out_grads[0]
    shard_rows = master.shape[1]
    width = master.shape[2]
    positions = jnp.arange(holders, dtype=jnp.int32)
    expert_id = jnp.sum(jnp.where(old_place == my_holder, selected, 0))
    table = jnp.arange(counts.shape[1], dtype=jnp.int32)
    routed = jnp.sum(jnp.where(table == expert_id, counts[0], 0))
    live = jnp.arange(tokens_here.shape[0], dtype=jnp.int32) < routed
    masked = jnp.where(live[:, None], grads_here, jnp.zeros_like(grads_here))
    destination = jnp.sum(
        jnp.where(old_place[None, :] == positions[:, None], new_place[None, :], 0), axis=1
    )
    order = jnp.sum(
        jnp.where(destination[None, :] == positions[:, None], positions[None, :], 0), axis=1
    )
    groups = lax.axis_size("dp")
    rows_each = tokens_here.shape[0]
    columns = lax.all_to_all(tokens_here, "dp", split_axis=1, concat_axis=0, tiled=True)
    every = lax.all_gather(masked, "dp", axis=0, tiled=True)
    blocks = jnp.einsum(
        "stk,stf->skf",
        columns.reshape(groups, rows_each, shard_rows),
        every.reshape(groups, rows_each, width),
        preferred_element_type=jnp.float32,
    )
    rounded = lax.optimization_barrier(blocks.astype(jnp.bfloat16))
    gradient = jnp.sum(rounded.astype(jnp.float32), axis=0)
    updated = adamw(master[0], first_moment[0], second_moment[0], gradient)
    weights, moment_one, moment_two = relocate_states(updated[0], updated[1], updated[2], order)
    lowered = weights.astype(jnp.bfloat16)
    incoming = next_tokens[0]
    columns = incoming
    forward = jnp.dot(
        columns,
        lax.all_gather(lowered, "dp", axis=0, tiled=True),
        preferred_element_type=jnp.float32,
    )
    return (weights[None], moment_one[None], moment_two[None], forward.astype(jnp.bfloat16)[None])


def solution(mesh):
    chips = mesh.shape["expert"] // CORES
    few = mesh.shape["expert"] % CORES == 0 and math.factorial(chips) <= ROUTE_LIMIT
    return jax.shard_map(
        direct_body if few else relay_body,
        mesh=mesh,
        in_specs=(
            P("expert", "dp", None),
            P("expert", "dp", None),
            P("expert", "dp", None),
            P("expert", "dp", None),
            P("expert", "dp", None),
            P("expert", "dp", None),
            P("dp", None),
            P(),
            P(),
            P(),
        ),
        out_specs=(
            P("expert", "dp", None),
            P("expert", "dp", None),
            P("expert", "dp", None),
            P("expert", "dp", None),
        ),
        check_vma=False,
    )
```
